32 devices in a mesh: trait: 2 (over x), ppl: 16 (over z, y, core).
Axes of the slice: x: 2, y: 2, z: 4, core: 2. Of those that a mesh axis runs over, the one named last changes fastest.
Arguments:
- genotypes: bfloat16 [8192, 4096], P(('trait', 'ppl')), parts along dimension 0
- residual: float32 [64, 4096], P('trait', 'ppl'), parts along dimension 0, may hold values from -36 to 36
- noise_people: float32 [64, 4096], P('trait', 'ppl'), parts along dimension 0, may hold values from -6 to 6
- noise_coef: float32 [64, 4096], P('trait'), parts along dimension 0, may hold values from -6 to 6
- coef_all: float32 [64, 8192], P('trait'), parts along dimension 0, may hold values from -0.06 to 0.06
- block_index: int32 [2], P('trait'), parts along dimension 0, may hold values from 0 to 1
- prior_prec: float32 [64], P('trait'), parts along dimension 0, may hold values from 21 to 103
- sigma2_old: float32 [64], P('trait'), parts along dimension 0, may hold values from 0.5 to 2
- gamma_draw: float32 [64], P('trait'), parts along dimension 0, may hold values from 0.8 to 1.25
- valid_counts: int32 [32], P('trait'), parts along dimension 0, may hold values from 128 to 256, as said below
Outputs:
- coef_new: float32 [64, 8192], P('trait'), parts along dimension 0
- residual_new: float32 [64, 4096], P('trait', 'ppl'), parts along dimension 0
- sigma2_new: float32 [64], P('trait'), parts along dimension 0
The draws below stay inside these ranges and needn't reach their ends.
There are 2 independent parts, one for each index of `trait`. The reference program is written for one: setup_inputs(seed, part) draws one part's arguments, and reference() takes and returns one part's arrays. A program takes and returns all parts, laid end to end along the dimension named above; each array names one. Nothing has to cross between parts.
Inputs may be any that keep to these rules, and one draw needn't show every extreme that they name: `valid_counts`: each entry counts the people present in one device's 256 slots; they fill the lowest slots, and some entry equals 256.
All inputs are finite; a program needn't handle non-finite values.
Results may differ from the reference program's by a relative error of at most 0.0049.
Values may be sent and summed in bfloat16 or wider, within the bound.
A program may use at most 64 MiB of HBM per device.

```python
import math
import jax
import jax.numpy as jnp
from jax import lax

ROWS_DEV = 256
BATCH = 4096
TRAITS = 32
ITERS = 4
BLOCKS = 2
PEOPLE = 4096
VARS = 8192
N_PPL = 16


def draw_genotypes(key, part):
    inner_key = jax.random.fold_in(key, 11)
    innov = jax.random.normal(inner_key, (PEOPLE, BATCH + 2), jnp.float32)
    blended = innov[:, 1:-1] + 0.45 * (innov[:, :-2] + innov[:, 2:])
    return (blended / jnp.sqrt(1.405)).astype(jnp.bfloat16)


def draw_residual(key, part):
    inner_key = jax.random.fold_in(key, 23)
    position = jnp.arange(PEOPLE, dtype=jnp.float32) / PEOPLE
    base = jax.random.normal(inner_key, (TRAITS, PEOPLE), jnp.float32)
    scale_line = 1.0 + 2.0 * position
    return jnp.clip(base, -6.0, 6.0) * scale_line[None, :]


def draw_valid_counts(key, part):
    inner_key = jax.random.fold_in(key, 7)
    key_counts, key_full = jax.random.split(inner_key)
    drawn_counts = jax.random.randint(key_counts, (N_PPL,), ROWS_DEV // 2, ROWS_DEV + 1)
    full_shard = jax.random.randint(key_full, (), 0, N_PPL)
    filled = jnp.where(jnp.arange(N_PPL) == full_shard, ROWS_DEV, drawn_counts)
    return filled.astype(jnp.int32)


def levels(rng, dims, cuts, low, high):
    factor_of, own = 1.0, jax.random.fold_in(rng, 6)
    for dim, blocks in cuts:
        steps = jnp.exp(jax.random.uniform(jax.random.fold_in(own, dim), (blocks,), jnp.float32, low / len(cuts), high / len(cuts)))
        factor_of = factor_of * jnp.repeat(steps, dims[dim] // blocks).reshape([-1 if axis == dim else 1 for axis in range(len(dims))])
    return factor_of


def normal_values(stream_key, extent, scale, limit, shards=(), kind=jnp.bfloat16):
    loudness = levels(stream_key, extent, shards, -0.22, 0.18) if shards else 1.0
    entries = jax.random.normal(stream_key, extent, jnp.float32) * scale * loudness
    return jnp.minimum(jnp.maximum(entries, -limit), limit).astype(kind)


def setup_inputs(seed: int = 0, part: int = 0) -> dict:
    seeds = jax.random.split(jax.random.key(seed), 11)
    own_keys = jax.random.split(jax.random.fold_in(seeds[10], part), 11)
    return {
        "genotypes": draw_genotypes(jax.random.fold_in(jax.random.fold_in(seeds[10], part), 71), part),
        "residual": draw_residual(jax.random.fold_in(jax.random.fold_in(seeds[10], part), 71), part),
        "noise_people": normal_values(own_keys[2], (TRAITS, PEOPLE), 1.0, 6.0, ((1, 16),), jnp.float32),
        "noise_coef": normal_values(own_keys[3], (TRAITS, BATCH), 1.0, 6.0, (), jnp.float32),
        "coef_all": normal_values(own_keys[4], (TRAITS, VARS), 0.01, 0.06, (), jnp.float32),
        "block_index": jax.random.randint(own_keys[5], (1,), 0, BLOCKS).astype(jnp.int32),
        "prior_prec": jnp.clip(jnp.exp(jax.random.uniform(own_keys[6], (TRAITS,), jnp.float32, math.log(21.0), math.log(103.0))), 21.0, 103.0),
        "sigma2_old": jnp.clip(jnp.exp(jax.random.uniform(own_keys[7], (TRAITS,), jnp.float32, math.log(0.5), math.log(2.0))), 0.5, 2.0),
        "gamma_draw": jnp.clip(jax.random.uniform(own_keys[8], (TRAITS,), jnp.float32, 0.8, 1.25), 0.8, 1.25),
        "valid_counts": draw_valid_counts(jax.random.fold_in(jax.random.fold_in(seeds[10], part), 71), part),
    }


PRIOR_DOF = 4.0
PRIOR_SCALE = 0.5

def reference(genotypes, residual, noise_people, noise_coef, coef_all, block_index, prior_prec, sigma2_old, gamma_draw, valid_counts):
    people_total = genotypes.shape[0]
    slot_ids = jnp.arange(people_total, dtype=jnp.int32)
    shard_ids = slot_ids // ROWS_DEV
    within = slot_ids % ROWS_DEV
    person_mask = (within < valid_counts[shard_ids]).astype(jnp.float32)[None, :]
    first_col = (block_index[0] * BATCH).astype(jnp.int32)
    old_coef = lax.dynamic_slice_in_dim(coef_all, first_col, BATCH, 1)
    contract = (((1,), (1,)), ((), ()))
    fitted_old = lax.dot_general(old_coef.astype(jnp.bfloat16), genotypes, contract, preferred_element_type=jnp.float32)
    partial_res = person_mask * (residual + fitted_old)
    noise_var = sigma2_old[:, None]
    ridge = prior_prec[:, None]
    target = (person_mask * (partial_res + jnp.sqrt(noise_var) * noise_people)).astype(jnp.bfloat16)
    rhs = jnp.dot(target, genotypes, preferred_element_type=jnp.float32) / noise_var + jnp.sqrt(ridge) * noise_coef
    batch_coef = jnp.zeros_like(rhs)
    fitted = jnp.zeros_like(partial_res)
    search = rhs
    direction = rhs
    norm_now = lax.optimization_barrier(jnp.sum(search * search, axis=1))
    for number in range(ITERS):
        dir_low = direction.astype(jnp.bfloat16)
        dir_full = lax.optimization_barrier(dir_low).astype(jnp.float32)
        image = person_mask * lax.dot_general(dir_low, genotypes, contract, preferred_element_type=jnp.float32)
        image_low = image.astype(jnp.bfloat16)
        applied = jnp.dot(image_low, genotypes, preferred_element_type=jnp.float32) / noise_var + ridge * dir_full
        step_size = norm_now / lax.optimization_barrier(jnp.sum(dir_full * applied, axis=1))
        batch_coef = batch_coef + step_size[:, None] * dir_full
        fitted = fitted + step_size[:, None] * image
        search = search - step_size[:, None] * applied
        norm_next = lax.optimization_barrier(jnp.sum(search * search, axis=1))
        direction = search + (norm_next / norm_now)[:, None] * direction
        norm_now = norm_next
    residual_new = partial_res - fitted
    squares = lax.optimization_barrier(jnp.sum(residual_new * residual_new, axis=1))
    present = jnp.sum(valid_counts).astype(jnp.float32)
    sigma2_new = (squares + PRIOR_DOF * PRIOR_SCALE) / ((present + PRIOR_DOF) * gamma_draw)
    coef_new = lax.dynamic_update_slice_in_dim(coef_all, batch_coef, first_col, 1)
    return (coef_new, residual_new, sigma2_new)
```

```python
import functools

import jax
import jax.numpy as jnp
from jax import lax
from jax.experimental import pallas as pl
from jax.experimental.pallas import tpu as pltpu
from jax.sharding import PartitionSpec as P

ITERS = 4
PRIOR_DOF = 4.0
PRIOR_SCALE = 0.5
NT = (((1,), (1,)), ((), ()))
NN = (((1,), (0,)), ((), ()))
LANES = 128
F32 = jnp.float32
BF16 = jnp.bfloat16


def kernel(
    n,
    owners,
    block_ref,
    counts_ref,
    prior_ref,
    sigma_ref,
    gamma_ref,
    res_ref,
    noise_p_ref,
    noise_c_ref,
    coef_all_ref,
    geno_ref,
    coef_out,
    res_out,
    sigma_out,
    g,
    g_other,
    coef_v,
    noise_c,
    dir_low,
    dir_full,
    coef,
    search,
    t_send,
    t_recv,
    r_send,
    r_recv,
    x_send,
    x_recv,
    rs_send,
    rs_recv,
    first_send,
    first_recv,
    pd_send,
    pd_recv,
    ag_send,
    ag_recv,
    sc_send,
    sc_recv,
    f_recv,
    e_recv,
    ed_recv,
    loc_sem,
    pair_send,
    pair_recv,
    rs_ssem,
    rs_rsem,
    pd_ssem,
    pd_rsem,
    ag_ssem,
    ag_rsem,
    sc_ssem,
    sc_rsem,
    f_ssem,
    f_rsem,
):
    rows, batch = geno_ref.shape
    traits, width = coef_all_ref.shape
    half = batch // 2
    people = 2 * rows
    chips = n // 2
    chunk = half // owners
    first = (chips - owners) // 2
    me = lax.axis_index("ppl")
    chip = lax.div(me, 2)
    core = lax.rem(me, 2)
    mate = me + 1 - 2 * core
    mine = pl.multiple_of(core * half, LANES)
    theirs = pl.multiple_of((1 - core) * half, LANES)
    my_rows = pl.multiple_of(core * rows, rows)
    owner = jnp.logical_and(chip >= first, chip < first + owners)
    own = jnp.clip(chip - first, 0, owners - 1)
    own_col = pl.multiple_of(own * chunk, LANES)

    def remote(src, dst, send, recv, target):
        return pltpu.make_async_remote_copy(
            src_ref=src,
            dst_ref=dst,
            send_sem=send,
            recv_sem=recv,
            device_id={"ppl": target},
            device_id_type=pl.DeviceIdType.MESH,
        )

    load_coef = pltpu.make_async_copy(coef_all_ref, coef_v, loc_sem.at[0])
    load_mine = pltpu.make_async_copy(
        geno_ref.at[:, pl.ds(mine, half)], g.at[pl.ds(my_rows, rows), :], loc_sem.at[1]
    )
    load_other = pltpu.make_async_copy(geno_ref.at[:, pl.ds(theirs, half)], g_other, loc_sem.at[2])
    load_noise = pltpu.make_async_copy(
        noise_c_ref.at[:, pl.ds(pl.multiple_of(mine + own_col, LANES), chunk)], noise_c, loc_sem.at[3]
    )
    load_other.start()
    load_coef.start()
    load_mine.start()
    load_noise.start()

    barrier = pltpu.get_barrier_semaphore()

    @pl.loop(1, n)
    def _(step):
        pl.semaphore_signal(
            barrier,
            inc=1,
            device_id={"ppl": lax.rem(me + step, n)},
            device_id_type=pl.DeviceIdType.MESH,
        )

    row_id = lax.broadcasted_iota(jnp.int32, (traits, LANES), 0)
    lane_id = lax.broadcasted_iota(jnp.int32, (traits, LANES), 1)

    def to_row(column, kind):
        spread = jnp.where(lane_id == row_id + kind * traits, jnp.broadcast_to(column, (traits, LANES)), 0.0)
        return jnp.sum(spread, axis=0, keepdims=True)

    def to_col(row, kind):
        spread = jnp.where(lane_id == row_id + kind * traits, jnp.broadcast_to(row, (traits, LANES)), 0.0)
        return jnp.sum(spread, axis=1, keepdims=True)

    def small(ref):
        spread = jnp.where(
            lane_id[:, :traits] == row_id[:, :traits], jnp.broadcast_to(ref[...], (traits, traits)), 0.0
        )
        return jnp.sum(spread, axis=1, keepdims=True)

    noise_var = small(sigma_ref)
    ridge = small(prior_ref)

    def mask_of(device, size):
        return (lax.broadcasted_iota(jnp.int32, (1, size), 1) < counts_ref[device]).astype(F32)

    mask_own = mask_of(me, rows)
    mask = jnp.concatenate([mask_of(2 * chip, rows), mask_of(2 * chip + 1, rows)], axis=1)

    load_coef.wait()

    def old_part(offset):
        value = coef_v[:, pl.ds(offset, half)]
        for b in range(1, width // batch):
            value = jnp.where(
                block_ref[0] == b, coef_v[:, pl.ds(pl.multiple_of(offset + b * batch, LANES), half)], value
            )
        return value.astype(BF16)

    load_other.wait()
    pl.semaphore_wait(barrier, n - 1)
    g_copy = remote(g_other, g.at[pl.ds(my_rows, rows), :], pair_send.at[0], pair_recv.at[0], mate)
    g_copy.start()
    fitted_old = lax.dot_general(old_part(theirs), g_other[...], NT, preferred_element_type=F32)
    load_mine.wait()
    fitted_old = fitted_old + lax.dot_general(
        old_part(mine), g[pl.ds(my_rows, rows), :], NT, preferred_element_type=F32
    )
    partial = mask_own * (res_ref[...] + fitted_old)
    target = (mask_own * (partial + jnp.sqrt(noise_var) * noise_p_ref[...])).astype(BF16)
    t_send[...] = target
    r_send[...] = partial
    t_copy = remote(t_send, t_recv, pair_send.at[1], pair_recv.at[1], mate)
    r_copy = remote(r_send, r_recv, pair_send.at[2], pair_recv.at[2], mate)
    t_copy.start()
    r_copy.start()

    flip = jnp.where(chip < chips // 2, owners // 2, 0)

    def reduce_scatter(left, out, into):
        copies = []
        for i in range(owners):
            o = lax.rem(flip + i, owners)
            cols = pl.ds(pl.multiple_of(o * chunk, LANES), chunk)
            piece = lax.dot_general(left, g[:, cols], NN, preferred_element_type=F32)
            out[o] = piece.astype(out.dtype)
            copy = remote(
                out.at[o], into.at[chip], rs_ssem.at[o], rs_rsem.at[chip], 2 * (o + first) + core
            )

            @pl.when(o + first != chip)
            def _():
                copy.start()

            copies.append((o, copy))
        return copies

    def owner_sum(out, into):
        for k in range(chips):

            @pl.when(chip != k)
            def _():
                remote(out.at[0], into.at[k], rs_ssem.at[0], rs_rsem.at[k], me).wait_recv()

        into[chip] = out[own]
        total = into[0].astype(F32)
        for k in range(1, chips):
            total = total + into[k].astype(F32)
        return total

    def pd_copy(o, slot):
        return remote(
            pd_send.at[pl.ds(0, 1), :],
            pd_recv.at[slot, pl.ds(0, 1), :],
            pd_ssem.at[o],
            pd_rsem.at[slot],
            2 * (o + first) + core,
        )

    def send_pd(row):
        pd_send[0:1, :] = row
        for o in range(owners):

            @pl.when(o + first != chip)
            def _():
                pd_copy(o, chip).start()

    def owner_pd():
        for k in range(chips):

            @pl.when(chip != k)
            def _():
                pd_copy(0, k).wait_recv()

        pd_recv[chip, 0:1, :] = pd_send[0:1, :]
        total = pd_recv[0, 0:1, :]
        for k in range(1, chips):
            total = total + pd_recv[k, 0:1, :]
        return total

    def ag_copy(slot, k):
        return remote(ag_send, ag_recv.at[slot], ag_ssem.at[k], ag_rsem.at[slot], 2 * k + core)

    def sc_copy(slot, d):
        return remote(
            sc_send.at[pl.ds(0, 1), :], sc_recv.at[slot, pl.ds(0, 1), :], sc_ssem.at[d], sc_rsem.at[slot], d
        )

    def owner_gather(row):
        ag_send[...] = search[...].astype(BF16)
        sc_send[0:1, :] = row
        slot = 2 * own + core
        for i in range(chips):
            k = (i // 2 if i % 2 == 0 else chips - 1 - i // 2)

            @pl.when(chip != k)
            def _():
                ag_copy(own, k).start()

        for d in range(n):

            @pl.when(me != d)
            def _():
                sc_copy(slot, d).start()

        ag_recv[own] = ag_send[...]
        sc_recv[slot, 0:1, :] = row

    def finish(copies, with_pd):
        for o, copy in copies:

            @pl.when(o + first != chip)
            def _():
                copy.wait_send()

        if with_pd:
            for o in range(owners):

                @pl.when(o + first != chip)
                def _():
                    pd_copy(o, chip).wait_send()

        @pl.when(owner)
        def _():
            for k in range(chips):

                @pl.when(chip != k)
                def _():
                    ag_copy(own, k).wait_send()

            for d in range(n):

                @pl.when(me != d)
                def _():
                    sc_copy(2 * own + core, d).wait_send()

    def wait_gather():
        for o in range(owners):
            for c in range(2):

                @pl.when(jnp.logical_or(o + first != chip, c != core))
                def _():
                    sc_copy(2 * o + c, 0).wait_recv()

        for o in range(owners):

            @pl.when(o + first != chip)
            def _():
                ag_copy(o, 0).wait_recv()

        total = sc_recv[0, 0:1, :]
        for s in range(1, 2 * owners):
            total = total + sc_recv[s, 0:1, :]
        return total, sc_recv[0, 0:1, :]

    t_copy.wait()
    g_copy.wait()
    targets = jnp.concatenate(
        [
            jnp.where(core == 0, target, t_recv[...]),
            jnp.where(core == 0, t_recv[...], target),
        ],
        axis=1,
    )
    copies = reduce_scatter(targets, first_send, first_recv)

    load_noise.wait()

    @pl.when(owner)
    def _():
        rhs = owner_sum(first_send, first_recv) / noise_var + jnp.sqrt(ridge) * noise_c[...]
        search[...] = rhs
        owner_gather(to_row(jnp.sum(rhs * rhs, axis=1, keepdims=True), 0))

    r_copy.wait()
    residual = jnp.concatenate(
        [
            jnp.where(core == 0, partial, r_recv[...]),
            jnp.where(core == 0, r_recv[...], partial),
        ],
        axis=1,
    )
    totals, _unused = wait_gather()
    norm = to_col(totals, 0)
    for o in range(owners):
        dir_low[:, o * chunk : (o + 1) * chunk] = ag_recv[o]
        dir_full[:, o * chunk : (o + 1) * chunk] = ag_recv[o].astype(F32)
    coef[...] = jnp.zeros_like(coef)
    finish(copies, False)

    for number in range(ITERS):
        last = number == ITERS - 1
        low = dir_low[...]
        wide = low.astype(F32)
        image_part = lax.dot_general(low, g[...], NT, preferred_element_type=F32)
        sq_part = jnp.sum(wide * wide, axis=1, keepdims=True)
        x_send[:, :people] = image_part
        x_send[:, people:] = jnp.broadcast_to(sq_part, (traits, LANES))
        x_copy = remote(x_send, x_recv, pair_send.at[1], pair_recv.at[1], mate)
        x_copy.start()
        if last:
            e_copy = remote(coef, e_recv, pair_send.at[2], pair_recv.at[2], mate)
            d_copy = remote(dir_low, ed_recv, pair_send.at[3], pair_recv.at[3], mate)
            e_copy.start()
            d_copy.start()
        x_copy.wait()
        image = mask * (image_part + x_recv[:, :people])
        dir_sq = sq_part + x_recv[:, people : people + 1]
        image_low = image.astype(BF16)
        dot_row = to_row(jnp.sum(image_low.astype(F32) * image, axis=1, keepdims=True), 0)
        if not last:
            send_pd(dot_row)
            copies = reduce_scatter(image_low, rs_send, rs_recv)

            @pl.when(owner)
            def _():
                pd = to_col(owner_pd(), 0)
                step = norm / (pd / noise_var + ridge * dir_sq)
                applied = owner_sum(rs_send, rs_recv) / noise_var + ridge * dir_low[:, pl.ds(own_col, chunk)].astype(F32)
                fresh = search[...] - step * applied
                search[...] = fresh
                owner_gather(to_row(jnp.sum(fresh * fresh, axis=1, keepdims=True), 0) + to_row(step, 1))

            totals, head = wait_gather()
            norm_next = to_col(totals, 0)
            step = to_col(head, 1)
            ratio = norm_next / norm
            norm = norm_next
            coef[...] += step * wide
            residual = residual - step * image
            for o in range(owners):
                cols = slice(o * chunk, (o + 1) * chunk)
                fresh = ag_recv[o].astype(F32) + ratio * dir_full[:, cols]
                dir_full[:, cols] = fresh
                dir_low[:, cols] = fresh.astype(BF16)
            finish(copies, True)

    row = (
        dot_row
        + to_row(jnp.sum(residual * image, axis=1, keepdims=True), 1)
        + to_row(jnp.sum(residual * residual, axis=1, keepdims=True), 2)
        + to_row(jnp.sum(image * image, axis=1, keepdims=True), 3)
    )
    pd_send[0:1, :] = row

    def f_copy(slot, k):
        return remote(
            pd_send.at[pl.ds(0, 1), :], f_recv.at[slot, pl.ds(0, 1), :], f_ssem.at[k], f_rsem.at[slot], 2 * k + core
        )

    for k in range(chips):

        @pl.when(chip != k)
        def _():
            f_copy(chip, k).start()

    f_recv[chip, 0:1, :] = row
    e_copy.wait()
    d_copy.wait()
    for k in range(chips):

        @pl.when(chip != k)
        def _():
            f_copy(k, 0).wait_recv()

    total = f_recv[0, 0:1, :]
    for k in range(1, chips):
        total = total + f_recv[k, 0:1, :]
    step = norm / (to_col(total, 0) / noise_var + ridge * dir_sq)
    squares = to_col(total, 2) - 2.0 * step * to_col(total, 1) + step * step * to_col(total, 3)
    residual_new = residual - step * image
    res_out[...] = jnp.where(core == 0, residual_new[:, :rows], residual_new[:, rows:])
    present = counts_ref[0]
    for d in range(1, n):
        present = present + counts_ref[d]
    sigma = (squares + PRIOR_DOF * PRIOR_SCALE) / ((present.astype(F32) + PRIOR_DOF) * small(gamma_ref))
    sigma_out[...] = to_row(sigma, 0)
    coef_out[:, pl.ds(mine, half)] = coef[...] + step * wide
    coef_out[:, pl.ds(theirs, half)] = e_recv[...] + step * ed_recv[...].astype(F32)
    for k in range(chips):

        @pl.when(chip != k)
        def _():
            f_copy(chip, k).wait_send()


def per_device(
    n,
    genotypes,
    residual,
    noise_people,
    noise_coef,
    coef_all,
    block_index,
    prior_prec,
    sigma2_old,
    gamma_draw,
    valid_counts,
):
    rows, batch = genotypes.shape
    traits, width = coef_all.shape
    half = batch // 2
    people = 2 * rows
    chips = n // 2
    owners = max(1, min(chips // 2, half // LANES))
    chunk = half // owners
    vmem = pl.BlockSpec(memory_space=pltpu.VMEM)
    smem = pl.BlockSpec(memory_space=pltpu.SMEM)
    hbm = pl.BlockSpec(memory_space=pl.ANY)
    dma = pltpu.SemaphoreType.DMA
    batch_coef, residual_new, sigma = pl.pallas_call(
        functools.partial(kernel, n, owners),
        out_shape=(
            jax.ShapeDtypeStruct((traits, batch), F32),
            jax.ShapeDtypeStruct((traits, rows), F32),
            jax.ShapeDtypeStruct((1, LANES), F32),
        ),
        in_specs=[smem, smem, vmem, vmem, vmem, vmem, vmem, hbm, hbm, hbm],
        out_specs=(vmem, vmem, vmem),
        scratch_shapes=[
            pltpu.VMEM((people, half), BF16),
            pltpu.VMEM((rows, half), BF16),
            pltpu.VMEM((traits, width), F32),
            pltpu.VMEM((traits, chunk), F32),
            pltpu.VMEM((traits, half), BF16),
            pltpu.VMEM((traits, half), F32),
            pltpu.VMEM((traits, half), F32),
            pltpu.VMEM((traits, chunk), F32),
            pltpu.VMEM((traits, rows), BF16),
            pltpu.VMEM((traits, rows), BF16),
            pltpu.VMEM((traits, rows), F32),
            pltpu.VMEM((traits, rows), F32),
            pltpu.VMEM((traits, people + LANES), F32),
            pltpu.VMEM((traits, people + LANES), F32),
            pltpu.VMEM((owners, traits, chunk), BF16),
            pltpu.VMEM((chips, traits, chunk), BF16),
            pltpu.VMEM((owners, traits, chunk), F32),
            pltpu.VMEM((chips, traits, chunk), F32),
            pltpu.VMEM((8, LANES), F32),
            pltpu.VMEM((chips, 8, LANES), F32),
            pltpu.VMEM((traits, chunk), BF16),
            pltpu.VMEM((owners, traits, chunk), BF16),
            pltpu.VMEM((8, LANES), F32),
            pltpu.VMEM((2 * owners, 8, LANES), F32),
            pltpu.VMEM((chips, 8, LANES), F32),
            pltpu.VMEM((traits, half), F32),
            pltpu.VMEM((traits, half), BF16),
            dma((4,)),
            dma((4,)),
            dma((4,)),
            dma((owners,)),
            dma((chips,)),
            dma((owners,)),
            dma((chips,)),
            dma((chips,)),
            dma((owners,)),
            dma((n,)),
            dma((2 * owners,)),
            dma((chips,)),
            dma((chips,)),
        ],
        compiler_params=pltpu.CompilerParams(
            collective_id=0, has_side_effects=True, vmem_limit_bytes=40 * 1024 * 1024
        ),
    )(
        block_index,
        valid_counts,
        prior_prec[None, :],
        sigma2_old[None, :],
        gamma_draw[None, :],
        residual,
        noise_people,
        noise_coef,
        coef_all,
        genotypes,
    )
    coef_new = lax.dynamic_update_slice_in_dim(coef_all, batch_coef, block_index[0] * batch, 1)
    return (coef_new, residual_new, sigma[0, :traits])


def solution(mesh):
    return jax.shard_map(
        functools.partial(per_device, mesh.shape["ppl"]),
        mesh=mesh,
        in_specs=(
            P(("trait", "ppl"), None),
            P("trait", "ppl"),
            P("trait", "ppl"),
            P("trait", None),
            P("trait", None),
            P("trait"),
            P("trait"),
            P("trait"),
            P("trait"),
            P("trait"),
        ),
        out_specs=(P("trait", None), P("trait", "ppl"), P("trait")),
        check_vma=False,
    )
```

```python
import functools

import jax
import jax.numpy as jnp
from jax import lax
from jax.experimental import pallas as pl
from jax.experimental.pallas import tpu as pltpu
from jax.sharding import PartitionSpec as P

ITERS = 4
PRIOR_DOF = 4.0
PRIOR_SCALE = 0.5
NT = (((1,), (1,)), ((), ()))
NN = (((1,), (0,)), ((), ()))
LANES = 128
CODE_MAX = 32767.0
F32 = jnp.float32
BF16 = jnp.bfloat16


def kernel(
    n,
    owners,
    block_hbm,
    counts_hbm,
    prior_hbm,
    sigma_hbm,
    gamma_hbm,
    res_hbm,
    noise_p_hbm,
    noise_c_ref,
    coef_all_ref,
    geno_ref,
    coef_out,
    res_out,
    sigma_out,
    block_ref,
    counts_ref,
    prior_ref,
    sigma_ref,
    gamma_ref,
    res_ref,
    noise_p_ref,
    g,
    g_other,
    coef_v,
    noise_c,
    dir_low,
    dir_full,
    coef,
    search,
    t_send,
    t_recv,
    r_send,
    r_recv,
    x_send,
    x_recv,
    rs_send,
    rs_recv,
    first_send,
    first_recv,
    scale_send,
    pd_send,
    pd_recv,
    ag_send,
    ag_recv,
    sc_send,
    sc_recv,
    f_recv,
    e_recv,
    ed_recv,
    loc_sem,
    pair_send,
    pair_recv,
    rs_ssem,
    rs_rsem,
    pd_ssem,
    pd_rsem,
    ag_ssem,
    ag_rsem,
    sc_ssem,
    sc_rsem,
    f_ssem,
    f_rsem,
):
    rows, batch = geno_ref.shape
    traits, width = coef_all_ref.shape
    half = batch // 2
    people = 2 * rows
    chips = n // 2
    chunk = half // owners
    first = (chips - owners) // 2
    me = lax.axis_index("ppl")
    chip = lax.div(me, 2)
    core = lax.rem(me, 2)
    mate = me + 1 - 2 * core
    mine = pl.multiple_of(core * half, LANES)
    theirs = pl.multiple_of((1 - core) * half, LANES)
    my_rows = pl.multiple_of(core * rows, rows)
    owner = jnp.logical_and(chip >= first, chip < first + owners)
    own = jnp.clip(chip - first, 0, owners - 1)
    own_col = pl.multiple_of(own * chunk, LANES)

    def remote(src, dst, send, recv, target):
        return pltpu.make_async_remote_copy(
            src_ref=src,
            dst_ref=dst,
            send_sem=send,
            recv_sem=recv,
            device_id={"ppl": target},
            device_id_type=pl.DeviceIdType.MESH,
        )

    load_coef = pltpu.make_async_copy(coef_all_ref, coef_v, loc_sem.at[0])
    load_mine = pltpu.make_async_copy(
        geno_ref.at[:, pl.ds(mine, half)], g.at[pl.ds(my_rows, rows), :], loc_sem.at[1]
    )
    load_other = pltpu.make_async_copy(geno_ref.at[:, pl.ds(theirs, half)], g_other, loc_sem.at[2])
    load_noise = pltpu.make_async_copy(
        noise_c_ref.at[:, pl.ds(pl.multiple_of(mine + own_col, LANES), chunk)], noise_c, loc_sem.at[3]
    )
    small_loads = [
        pltpu.make_async_copy(src, dst, loc_sem.at[4 + i])
        for i, (src, dst) in enumerate(
            (
                (counts_hbm, counts_ref),
                (block_hbm, block_ref),
                (prior_hbm, prior_ref),
                (sigma_hbm, sigma_ref),
                (gamma_hbm, gamma_ref),
                (res_hbm, res_ref),
                (noise_p_hbm, noise_p_ref),
            )
        )
    ]
    barrier = pltpu.get_barrier_semaphore()

    @pl.loop(1, n)
    def _(step):
        pl.semaphore_signal(
            barrier,
            inc=1,
            device_id={"ppl": lax.rem(me + step, n)},
            device_id_type=pl.DeviceIdType.MESH,
        )

    load_other.start()
    load_coef.start()
    for load in small_loads:
        load.start()
    load_mine.start()
    load_noise.start()

    row_id = lax.broadcasted_iota(jnp.int32, (traits, LANES), 0)
    lane_id = lax.broadcasted_iota(jnp.int32, (traits, LANES), 1)

    def to_row(column, kind):
        spread = jnp.where(lane_id == row_id + kind * traits, jnp.broadcast_to(column, (traits, LANES)), 0.0)
        return jnp.sum(spread, axis=0, keepdims=True)

    def to_col(row, kind):
        spread = jnp.where(lane_id == row_id + kind * traits, jnp.broadcast_to(row, (traits, LANES)), 0.0)
        return jnp.sum(spread, axis=1, keepdims=True)

    def small(ref):
        spread = jnp.where(
            lane_id[:, :traits] == row_id[:, :traits], jnp.broadcast_to(ref[...], (traits, traits)), 0.0
        )
        return jnp.sum(spread, axis=1, keepdims=True)

    for load in small_loads:
        load.wait()

    noise_var = small(sigma_ref)
    ridge = small(prior_ref)

    def mask_of(device, size):
        return (lax.broadcasted_iota(jnp.int32, (1, size), 1) < counts_ref[device]).astype(F32)

    mask_own = mask_of(me, rows)
    mask = jnp.concatenate([mask_of(2 * chip, rows), mask_of(2 * chip + 1, rows)], axis=1)

    load_coef.wait()

    def old_part(offset):
        value = coef_v[:, pl.ds(offset, half)]
        for b in range(1, width // batch):
            value = jnp.where(
                block_ref[0] == b, coef_v[:, pl.ds(pl.multiple_of(offset + b * batch, LANES), half)], value
            )
        return value.astype(BF16)

    load_other.wait()
    fitted_old = lax.dot_general(old_part(theirs), g_other[...], NT, preferred_element_type=F32)
    pl.semaphore_wait(barrier, n - 1)
    g_copy = remote(g_other, g.at[pl.ds(my_rows, rows), :], pair_send.at[0], pair_recv.at[0], mate)
    g_copy.start()
    load_mine.wait()
    fitted_old = fitted_old + lax.dot_general(
        old_part(mine), g[pl.ds(my_rows, rows), :], NT, preferred_element_type=F32
    )
    partial = mask_own * (res_ref[...] + fitted_old)
    target = (mask_own * (partial + jnp.sqrt(noise_var) * noise_p_ref[...])).astype(BF16)
    t_send[...] = target
    r_send[...] = partial
    t_copy = remote(t_send, t_recv, pair_send.at[1], pair_recv.at[1], mate)
    r_copy = remote(r_send, r_recv, pair_send.at[2], pair_recv.at[2], mate)
    t_copy.start()
    r_copy.start()

    flip = jnp.where(chip < chips // 2, owners // 2, 0)

    def scale_copy(o, slot):
        return remote(
            scale_send.at[o, pl.ds(0, 1), :],
            pd_recv.at[slot, pl.ds(0, 1), :],
            pd_ssem.at[o],
            pd_rsem.at[slot],
            2 * (o + first) + core,
        )

    def reduce_scatter(left, out, into, coded):
        copies = []
        for i in range(owners):
            o = lax.rem(flip + i, owners)
            cols = pl.ds(pl.multiple_of(o * chunk, LANES), chunk)
            piece = lax.dot_general(left, g[:, cols], NN, preferred_element_type=F32)
            if coded:
                peak = jnp.max(jnp.abs(piece), axis=1, keepdims=True)
                gain = jnp.where(peak > 1e-30, CODE_MAX / jnp.maximum(peak, 1e-30), 0.0)
                out[o] = jnp.round(piece * gain).astype(jnp.int32).astype(out.dtype)
                scale_send[o, 0:1, :] = to_row(peak * (1.0 / CODE_MAX), 0)

                @pl.when(o + first != chip)
                def _():
                    scale_copy(o, chip).start()

            else:
                out[o] = piece.astype(out.dtype)
            copy = remote(
                out.at[o], into.at[chip], rs_ssem.at[o], rs_rsem.at[chip], 2 * (o + first) + core
            )

            @pl.when(o + first != chip)
            def _():
                copy.start()

            copies.append((o, copy))
        return copies

    def owner_sum(out, into, coded):
        for k in range(chips):

            @pl.when(chip != k)
            def _():
                remote(out.at[0], into.at[k], rs_ssem.at[0], rs_rsem.at[k], me).wait_recv()
                if coded:
                    scale_copy(0, k).wait_recv()

        into[chip] = out[own]
        if coded:
            pd_recv[chip, 0:1, :] = scale_send[own, 0:1, :]

        def term(k):
            if coded:
                return into[k].astype(jnp.int32).astype(F32) * to_col(pd_recv[k, 0:1, :], 0)
            return into[k].astype(F32)

        total = term(0)
        for k in range(1, chips):
            total = total + term(k)
        return total

    def pd_copy(o, slot):
        return remote(
            pd_send.at[pl.ds(0, 1), :],
            pd_recv.at[slot, pl.ds(0, 1), :],
            pd_ssem.at[o],
            pd_rsem.at[slot],
            2 * (o + first) + core,
        )

    def send_pd(row):
        pd_send[0:1, :] = row
        for o in range(owners):

            @pl.when(o + first != chip)
            def _():
                pd_copy(o, chip).start()

    def owner_pd():
        for k in range(chips):

            @pl.when(chip != k)
            def _():
                pd_copy(0, k).wait_recv()

        pd_recv[chip, 0:1, :] = pd_send[0:1, :]
        total = pd_recv[0, 0:1, :]
        for k in range(1, chips):
            total = total + pd_recv[k, 0:1, :]
        return total

    def ag_copy(slot, k):
        return remote(ag_send, ag_recv.at[slot], ag_ssem.at[k], ag_rsem.at[slot], 2 * k + core)

    def sc_copy(slot, d):
        return remote(
            sc_send.at[pl.ds(0, 1), :], sc_recv.at[slot, pl.ds(0, 1), :], sc_ssem.at[d], sc_rsem.at[slot], d
        )

    def owner_gather(row):
        ag_send[...] = search[...].astype(BF16)
        sc_send[0:1, :] = row
        slot = 2 * own + core
        for i in range(chips):
            k = (i // 2 if i % 2 == 0 else chips - 1 - i // 2)

            @pl.when(chip != k)
            def _():
                ag_copy(own, k).start()

        for d in range(n):

            @pl.when(me != d)
            def _():
                sc_copy(slot, d).start()

        ag_recv[own] = ag_send[...]
        sc_recv[slot, 0:1, :] = row

    def finish(copies, row_copy):
        for o, copy in copies:

            @pl.when(o + first != chip)
            def _():
                copy.wait_send()

        for o in range(owners):

            @pl.when(o + first != chip)
            def _():
                row_copy(o, chip).wait_send()

        @pl.when(owner)
        def _():
            for k in range(chips):

                @pl.when(chip != k)
                def _():
                    ag_copy(own, k).wait_send()

            for d in range(n):

                @pl.when(me != d)
                def _():
                    sc_copy(2 * own + core, d).wait_send()

    def wait_gather():
        for o in range(owners):
            for c in range(2):

                @pl.when(jnp.logical_or(o + first != chip, c != core))
                def _():
                    sc_copy(2 * o + c, 0).wait_recv()

        for o in range(owners):

            @pl.when(o + first != chip)
            def _():
                ag_copy(o, 0).wait_recv()

        total = sc_recv[0, 0:1, :]
        for s in range(1, 2 * owners):
            total = total + sc_recv[s, 0:1, :]
        return total, sc_recv[0, 0:1, :]

    t_copy.wait()
    g_copy.wait()
    targets = jnp.concatenate(
        [
            jnp.where(core == 0, target, t_recv[...]),
            jnp.where(core == 0, t_recv[...], target),
        ],
        axis=1,
    )
    copies = reduce_scatter(targets, first_send, first_recv, True)

    load_noise.wait()

    @pl.when(owner)
    def _():
        rhs = owner_sum(first_send, first_recv, True) / noise_var + jnp.sqrt(ridge) * noise_c[...]
        search[...] = rhs
        owner_gather(to_row(jnp.sum(rhs * rhs, axis=1, keepdims=True), 0))

    r_copy.wait()
    residual = jnp.concatenate(
        [
            jnp.where(core == 0, partial, r_recv[...]),
            jnp.where(core == 0, r_recv[...], partial),
        ],
        axis=1,
    )
    totals, _unused = wait_gather()
    norm = to_col(totals, 0)
    for o in range(owners):
        dir_low[:, o * chunk : (o + 1) * chunk] = ag_recv[o]
        dir_full[:, o * chunk : (o + 1) * chunk] = ag_recv[o].astype(F32)
    coef[...] = jnp.zeros_like(coef)
    finish(copies, scale_copy)

    for number in range(ITERS):
        last = number == ITERS - 1
        low = dir_low[...]
        wide = low.astype(F32)
        image_part = lax.dot_general(low, g[...], NT, preferred_element_type=F32)
        sq_part = jnp.sum(wide * wide, axis=1, keepdims=True)
        x_send[:, :people] = image_part
        x_send[:, people:] = jnp.broadcast_to(sq_part, (traits, LANES))
        x_copy = remote(x_send, x_recv, pair_send.at[1], pair_recv.at[1], mate)
        x_copy.start()
        if last:
            e_copy = remote(coef, e_recv, pair_send.at[2], pair_recv.at[2], mate)
            d_copy = remote(dir_low, ed_recv, pair_send.at[3], pair_recv.at[3], mate)
            e_copy.start()
            d_copy.start()
        x_copy.wait()
        image = mask * (image_part + x_recv[:, :people])
        dir_sq = sq_part + x_recv[:, people : people + 1]
        image_low = image.astype(BF16)
        dot_row = to_row(jnp.sum(image_low.astype(F32) * image, axis=1, keepdims=True), 0)
        if not last:
            send_pd(dot_row)
            copies = reduce_scatter(image_low, rs_send, rs_recv, False)

            @pl.when(owner)
            def _():
                pd = to_col(owner_pd(), 0)
                step = norm / (pd / noise_var + ridge * dir_sq)
                applied = owner_sum(rs_send, rs_recv, False) / noise_var + ridge * dir_low[:, pl.ds(own_col, chunk)].astype(F32)
                fresh = search[...] - step * applied
                search[...] = fresh
                owner_gather(to_row(jnp.sum(fresh * fresh, axis=1, keepdims=True), 0) + to_row(step, 1))

            totals, head = wait_gather()
            norm_next = to_col(totals, 0)
            step = to_col(head, 1)
            ratio = norm_next / norm
            norm = norm_next
            coef[...] += step * wide
            residual = residual - step * image
            for o in range(owners):
                cols = slice(o * chunk, (o + 1) * chunk)
                fresh = ag_recv[o].astype(F32) + ratio * dir_full[:, cols]
                dir_full[:, cols] = fresh
                dir_low[:, cols] = fresh.astype(BF16)
            finish(copies, pd_copy)

    row = (
        dot_row
        + to_row(jnp.sum(residual * image, axis=1, keepdims=True), 1)
        + to_row(jnp.sum(residual * residual, axis=1, keepdims=True), 2)
        + to_row(jnp.sum(image * image, axis=1, keepdims=True), 3)
    )
    pd_send[0:1, :] = row

    def f_copy(slot, k):
        return remote(
            pd_send.at[pl.ds(0, 1), :], f_recv.at[slot, pl.ds(0, 1), :], f_ssem.at[k], f_rsem.at[slot], 2 * k + core
        )

    for k in range(chips):

        @pl.when(chip != k)
        def _():
            f_copy(chip, k).start()

    f_recv[chip, 0:1, :] = row
    e_copy.wait()
    d_copy.wait()
    for k in range(chips):

        @pl.when(chip != k)
        def _():
            f_copy(k, 0).wait_recv()

    total = f_recv[0, 0:1, :]
    for k in range(1, chips):
        total = total + f_recv[k, 0:1, :]
    step = norm / (to_col(total, 0) / noise_var + ridge * dir_sq)
    squares = to_col(total, 2) - 2.0 * step * to_col(total, 1) + step * step * to_col(total, 3)
    residual_new = residual - step * image
    res_out[...] = jnp.where(core == 0, residual_new[:, :rows], residual_new[:, rows:])
    present = counts_ref[0]
    for d in range(1, n):
        present = present + counts_ref[d]
    sigma = (squares + PRIOR_DOF * PRIOR_SCALE) / ((present.astype(F32) + PRIOR_DOF) * small(gamma_ref))
    sigma_out[...] = to_row(sigma, 0)[:, :traits]
    new_mine = coef[...] + step * wide
    new_theirs = e_recv[...] + step * ed_recv[...].astype(F32)
    for b in range(width // batch):
        for offset, value in ((mine, new_mine), (theirs, new_theirs)):
            cols = pl.ds(pl.multiple_of(offset + b * batch, LANES), half)
            coef_out[:, cols] = jnp.where(block_ref[0] == b, value, coef_v[:, cols])
    for k in range(chips):

        @pl.when(chip != k)
        def _():
            f_copy(chip, k).wait_send()


def per_device(
    n,
    genotypes,
    residual,
    noise_people,
    noise_coef,
    coef_all,
    block_index,
    prior_prec,
    sigma2_old,
    gamma_draw,
    valid_counts,
):
    rows, batch = genotypes.shape
    traits, width = coef_all.shape
    half = batch // 2
    people = 2 * rows
    chips = n // 2
    owners = max(1, min(chips // 2, half // LANES))
    chunk = half // owners
    vmem = pl.BlockSpec(memory_space=pltpu.VMEM)
    hbm = pl.BlockSpec(memory_space=pltpu.HBM)
    dma = pltpu.SemaphoreType.DMA
    coef_new, residual_new, sigma = pl.pallas_call(
        functools.partial(kernel, n, owners),
        out_shape=(
            jax.ShapeDtypeStruct((traits, width), F32),
            jax.ShapeDtypeStruct((traits, rows), F32),
            jax.ShapeDtypeStruct((1, traits), F32),
        ),
        in_specs=[hbm] * 10,
        out_specs=(vmem, vmem, vmem),
        scratch_shapes=[
            pltpu.SMEM(block_index.shape, jnp.int32),
            pltpu.SMEM(valid_counts.shape, jnp.int32),
            pltpu.VMEM((1, traits), F32),
            pltpu.VMEM((1, traits), F32),
            pltpu.VMEM((1, traits), F32),
            pltpu.VMEM((traits, rows), F32),
            pltpu.VMEM((traits, rows), F32),
            pltpu.VMEM((people, half), BF16),
            pltpu.VMEM((rows, half), BF16),
            pltpu.VMEM((traits, width), F32),
            pltpu.VMEM((traits, chunk), F32),
            pltpu.VMEM((traits, half), BF16),
            pltpu.VMEM((traits, half), F32),
            pltpu.VMEM((traits, half), F32),
            pltpu.VMEM((traits, chunk), F32),
            pltpu.VMEM((traits, rows), BF16),
            pltpu.VMEM((traits, rows), BF16),
            pltpu.VMEM((traits, rows), F32),
            pltpu.VMEM((traits, rows), F32),
            pltpu.VMEM((traits, people + LANES), F32),
            pltpu.VMEM((traits, people + LANES), F32),
            pltpu.VMEM((owners, traits, chunk), BF16),
            pltpu.VMEM((chips, traits, chunk), BF16),
            pltpu.VMEM((owners, traits, chunk), jnp.int16),
            pltpu.VMEM((chips, traits, chunk), jnp.int16),
            pltpu.VMEM((owners, 8, LANES), F32),
            pltpu.VMEM((8, LANES), F32),
            pltpu.VMEM((chips, 8, LANES), F32),
            pltpu.VMEM((traits, chunk), BF16),
            pltpu.VMEM((owners, traits, chunk), BF16),
            pltpu.VMEM((8, LANES), F32),
            pltpu.VMEM((2 * owners, 8, LANES), F32),
            pltpu.VMEM((chips, 8, LANES), F32),
            pltpu.VMEM((traits, half), F32),
            pltpu.VMEM((traits, half), BF16),
            dma((11,)),
            dma((4,)),
            dma((4,)),
            dma((owners,)),
            dma((chips,)),
            dma((owners,)),
            dma((chips,)),
            dma((chips,)),
            dma((owners,)),
            dma((n,)),
            dma((2 * owners,)),
            dma((chips,)),
            dma((chips,)),
        ],
        compiler_params=pltpu.CompilerParams(
            collective_id=0, has_side_effects=True, vmem_limit_bytes=60 * 1024 * 1024
        ),
    )(
        block_index,
        valid_counts,
        prior_prec[None, :],
        sigma2_old[None, :],
        gamma_draw[None, :],
        residual,
        noise_people,
        noise_coef,
        coef_all,
        genotypes,
    )
    return (coef_new, residual_new, sigma.reshape(traits))


def solution(mesh):
    return jax.shard_map(
        functools.partial(per_device, mesh.shape["ppl"]),
        mesh=mesh,
        in_specs=(
            P(("trait", "ppl"), None),
            P("trait", "ppl"),
            P("trait", "ppl"),
            P("trait", None),
            P("trait", None),
            P("trait"),
            P("trait"),
            P("trait"),
            P("trait"),
            P("trait"),
        ),
        out_specs=(P("trait", None), P("trait", "ppl"), P("trait")),
        check_vma=False,
    )
```

```python
import functools

import jax
import jax.numpy as jnp
from jax import lax
from jax.experimental import pallas as pl
from jax.experimental.pallas import tpu as pltpu
from jax.sharding import PartitionSpec as P

ITERS = 4
PRIOR_DOF = 4.0
PRIOR_SCALE = 0.5
NT = (((1,), (1,)), ((), ()))
NN = (((1,), (0,)), ((), ()))
LANES = 128
CODE_MAX = 32767.0
F32 = jnp.float32
BF16 = jnp.bfloat16


def kernel(
    n,
    owners,
    block_hbm,
    counts_hbm,
    prior_hbm,
    sigma_hbm,
    gamma_hbm,
    res_hbm,
    noise_p_hbm,
    noise_c_ref,
    coef_all_ref,
    geno_ref,
    coef_out,
    res_out,
    sigma_out,
    block_ref,
    counts_ref,
    prior_ref,
    sigma_ref,
    gamma_ref,
    res_ref,
    noise_p_ref,
    g,
    g_other,
    coef_v,
    noise_c,
    dir_low,
    dir_full,
    coef,
    search,
    t_send,
    t_recv,
    r_send,
    r_recv,
    x_send,
    x_recv,
    rs_send,
    rs_recv,
    first_send,
    first_recv,
    scale_send,
    pd_send,
    pd_recv,
    ag_send,
    ag_recv,
    sc_send,
    sc_recv,
    f_recv,
    e_recv,
    ed_recv,
    loc_sem,
    pair_send,
    pair_recv,
    rs_ssem,
    rs_rsem,
    pd_ssem,
    pd_rsem,
    ag_ssem,
    ag_rsem,
    sc_ssem,
    sc_rsem,
    f_ssem,
    f_rsem,
):
    rows, batch = geno_ref.shape
    traits, width = coef_all_ref.shape
    half = batch // 2
    people = 2 * rows
    chips = n // 2
    chunk = half // owners
    first = (chips - owners) // 2
    me = lax.axis_index("ppl")
    chip = lax.div(me, 2)
    core = lax.rem(me, 2)
    mate = me + 1 - 2 * core
    mine = pl.multiple_of(core * half, LANES)
    theirs = pl.multiple_of((1 - core) * half, LANES)
    my_rows = pl.multiple_of(core * rows, rows)
    owner = jnp.logical_and(chip >= first, chip < first + owners)
    own = jnp.clip(chip - first, 0, owners - 1)
    own_col = pl.multiple_of(own * chunk, LANES)

    def remote(src, dst, send, recv, target):
        return pltpu.make_async_remote_copy(
            src_ref=src,
            dst_ref=dst,
            send_sem=send,
            recv_sem=recv,
            device_id={"ppl": target},
            device_id_type=pl.DeviceIdType.MESH,
        )

    load_coef = pltpu.make_async_copy(coef_all_ref, coef_v, loc_sem.at[0])
    load_mine = pltpu.make_async_copy(
        geno_ref.at[:, pl.ds(mine, half)], g.at[pl.ds(my_rows, rows), :], loc_sem.at[1]
    )
    load_other = pltpu.make_async_copy(geno_ref.at[:, pl.ds(theirs, half)], g_other, loc_sem.at[2])
    load_noise = pltpu.make_async_copy(
        noise_c_ref.at[:, pl.ds(pl.multiple_of(mine + own_col, LANES), chunk)], noise_c, loc_sem.at[3]
    )
    small_loads = [
        pltpu.make_async_copy(src, dst, loc_sem.at[4 + i])
        for i, (src, dst) in enumerate(
            (
                (counts_hbm, counts_ref),
                (block_hbm, block_ref),
                (prior_hbm, prior_ref),
                (sigma_hbm, sigma_ref),
                (gamma_hbm, gamma_ref),
                (res_hbm, res_ref),
                (noise_p_hbm, noise_p_ref),
            )
        )
    ]
    barrier = pltpu.get_barrier_semaphore()

    @pl.loop(1, n)
    def _(step):
        pl.semaphore_signal(
            barrier,
            inc=1,
            device_id={"ppl": lax.rem(me + step, n)},
            device_id_type=pl.DeviceIdType.MESH,
        )

    load_other.start()
    load_coef.start()
    for load in small_loads:
        load.start()
    load_mine.start()
    load_noise.start()

    row_id = lax.broadcasted_iota(jnp.int32, (traits, LANES), 0)
    lane_id = lax.broadcasted_iota(jnp.int32, (traits, LANES), 1)

    def to_row(column, kind):
        spread = jnp.where(lane_id == row_id + kind * traits, jnp.broadcast_to(column, (traits, LANES)), 0.0)
        return jnp.sum(spread, axis=0, keepdims=True)

    def to_col(row, kind):
        spread = jnp.where(lane_id == row_id + kind * traits, jnp.broadcast_to(row, (traits, LANES)), 0.0)
        return jnp.sum(spread, axis=1, keepdims=True)

    def small(ref):
        spread = jnp.where(
            lane_id[:, :traits] == row_id[:, :traits], jnp.broadcast_to(ref[...], (traits, traits)), 0.0
        )
        return jnp.sum(spread, axis=1, keepdims=True)

    for load in small_loads:
        load.wait()

    noise_var = small(sigma_ref)
    ridge = small(prior_ref)

    def mask_of(device, size):
        return (lax.broadcasted_iota(jnp.int32, (1, size), 1) < counts_ref[device]).astype(F32)

    mask_own = mask_of(me, rows)
    mask = jnp.concatenate([mask_of(2 * chip, rows), mask_of(2 * chip + 1, rows)], axis=1)

    load_coef.wait()

    def old_part(offset):
        value = coef_v[:, pl.ds(offset, half)]
        for b in range(1, width // batch):
            value = jnp.where(
                block_ref[0] == b, coef_v[:, pl.ds(pl.multiple_of(offset + b * batch, LANES), half)], value
            )
        return value.astype(BF16)

    load_other.wait()
    fitted_old = lax.dot_general(old_part(theirs), g_other[...], NT, preferred_element_type=F32)
    pl.semaphore_wait(barrier, n - 1)
    g_copy = remote(g_other, g.at[pl.ds(my_rows, rows), :], pair_send.at[0], pair_recv.at[0], mate)
    g_copy.start()
    load_mine.wait()
    fitted_old = fitted_old + lax.dot_general(
        old_part(mine), g[pl.ds(my_rows, rows), :], NT, preferred_element_type=F32
    )
    partial = mask_own * (res_ref[...] + fitted_old)
    target = (mask_own * (partial + jnp.sqrt(noise_var) * noise_p_ref[...])).astype(BF16)
    t_send[...] = target
    r_send[...] = partial
    t_copy = remote(t_send, t_recv, pair_send.at[1], pair_recv.at[1], mate)
    r_copy = remote(r_send, r_recv, pair_send.at[2], pair_recv.at[2], mate)
    t_copy.start()
    r_copy.start()

    flip = jnp.where(chip < chips // 2, owners // 2, 0)

    def scale_copy(o, slot):
        return remote(
            scale_send.at[o, pl.ds(0, 1), :],
            pd_recv.at[slot, pl.ds(0, 1), :],
            pd_ssem.at[o],
            pd_rsem.at[slot],
            2 * (o + first) + core,
        )

    def reduce_scatter(left, out, into, coded):
        copies = []
        for i in range(owners):
            o = lax.rem(flip + i, owners)
            cols = pl.ds(pl.multiple_of(o * chunk, LANES), chunk)
            piece = lax.dot_general(left, g[:, cols], NN, preferred_element_type=F32)
            if coded:
                peak = jnp.max(jnp.abs(piece), axis=1, keepdims=True)
                gain = jnp.where(peak > 1e-30, CODE_MAX / jnp.maximum(peak, 1e-30), 0.0)
                out[o] = jnp.round(piece * gain).astype(jnp.int32).astype(out.dtype)
                scale_send[o, 0:1, :] = to_row(peak * (1.0 / CODE_MAX), 0)

                @pl.when(o + first != chip)
                def _():
                    scale_copy(o, chip).start()

            else:
                out[o] = piece.astype(out.dtype)
            copy = remote(
                out.at[o], into.at[chip], rs_ssem.at[o], rs_rsem.at[chip], 2 * (o + first) + core
            )

            @pl.when(o + first != chip)
            def _():
                copy.start()

            copies.append((o, copy))
        return copies

    def owner_sum(out, into, coded):
        for k in range(chips):

            @pl.when(chip != k)
            def _():
                remote(out.at[0], into.at[k], rs_ssem.at[0], rs_rsem.at[k], me).wait_recv()
                if coded:
                    scale_copy(0, k).wait_recv()

        into[chip] = out[own]
        if coded:
            pd_recv[chip, 0:1, :] = scale_send[own, 0:1, :]

        def term(k):
            if coded:
                return into[k].astype(jnp.int32).astype(F32) * to_col(pd_recv[k, 0:1, :], 0)
            return into[k].astype(F32)

        total = term(0)
        for k in range(1, chips):
            total = total + term(k)
        return total

    def pd_copy(o, slot):
        return remote(
            pd_send.at[pl.ds(0, 1), :],
            pd_recv.at[slot, pl.ds(0, 1), :],
            pd_ssem.at[o],
            pd_rsem.at[slot],
            2 * (o + first) + core,
        )

    def send_pd(row):
        pd_send[0:1, :] = row
        for o in range(owners):

            @pl.when(o + first != chip)
            def _():
                pd_copy(o, chip).start()

    def owner_pd():
        for k in range(chips):

            @pl.when(chip != k)
            def _():
                pd_copy(0, k).wait_recv()

        pd_recv[chip, 0:1, :] = pd_send[0:1, :]
        total = pd_recv[0, 0:1, :]
        for k in range(1, chips):
            total = total + pd_recv[k, 0:1, :]
        return total

    def ag_copy(slot, k):
        return remote(ag_send, ag_recv.at[slot], ag_ssem.at[k], ag_rsem.at[slot], 2 * k + core)

    def sc_copy(slot, d):
        return remote(
            sc_send.at[pl.ds(0, 1), :], sc_recv.at[slot, pl.ds(0, 1), :], sc_ssem.at[d], sc_rsem.at[slot], d
        )

    def owner_gather(row):
        ag_send[...] = search[...].astype(BF16)
        sc_send[0:1, :] = row
        slot = 2 * own + core
        for i in range(chips):
            k = (i // 2 if i % 2 == 0 else chips - 1 - i // 2)

            @pl.when(chip != k)
            def _():
                ag_copy(own, k).start()

        for d in range(n):

            @pl.when(me != d)
            def _():
                sc_copy(slot, d).start()

        ag_recv[own] = ag_send[...]
        sc_recv[slot, 0:1, :] = row

    def finish(copies, row_copy):
        for o, copy in copies:

            @pl.when(o + first != chip)
            def _():
                copy.wait_send()

        for o in range(owners):

            @pl.when(o + first != chip)
            def _():
                row_copy(o, chip).wait_send()

        @pl.when(owner)
        def _():
            for k in range(chips):

                @pl.when(chip != k)
                def _():
                    ag_copy(own, k).wait_send()

            for d in range(n):

                @pl.when(me != d)
                def _():
                    sc_copy(2 * own + core, d).wait_send()

    def wait_gather():
        for o in range(owners):
            for c in range(2):

                @pl.when(jnp.logical_or(o + first != chip, c != core))
                def _():
                    sc_copy(2 * o + c, 0).wait_recv()

        for o in range(owners):

            @pl.when(o + first != chip)
            def _():
                ag_copy(o, 0).wait_recv()

        total = sc_recv[0, 0:1, :]
        for s in range(1, 2 * owners):
            total = total + sc_recv[s, 0:1, :]
        return total, sc_recv[0, 0:1, :]

    t_copy.wait()
    g_copy.wait()
    targets = jnp.concatenate(
        [
            jnp.where(core == 0, target, t_recv[...]),
            jnp.where(core == 0, t_recv[...], target),
        ],
        axis=1,
    )
    copies = reduce_scatter(targets, first_send, first_recv, True)

    load_noise.wait()

    @pl.when(owner)
    def _():
        rhs = owner_sum(first_send, first_recv, True) / noise_var + jnp.sqrt(ridge) * noise_c[...]
        search[...] = rhs
        owner_gather(to_row(jnp.sum(rhs * rhs, axis=1, keepdims=True), 0))

    r_copy.wait()
    residual = jnp.concatenate(
        [
            jnp.where(core == 0, partial, r_recv[...]),
            jnp.where(core == 0, r_recv[...], partial),
        ],
        axis=1,
    )
    totals, _unused = wait_gather()
    norm = to_col(totals, 0)
    for o in range(owners):
        dir_low[:, o * chunk : (o + 1) * chunk] = ag_recv[o]
        dir_full[:, o * chunk : (o + 1) * chunk] = ag_recv[o].astype(F32)
    coef[...] = jnp.zeros_like(coef)
    finish(copies, scale_copy)

    for number in range(ITERS):
        last = number == ITERS - 1
        low = dir_low[...]
        wide = low.astype(F32)
        image_part = lax.dot_general(low, g[...], NT, preferred_element_type=F32)
        sq_part = jnp.sum(wide * wide, axis=1, keepdims=True)
        x_send[:, :people] = image_part
        x_send[:, people:] = jnp.broadcast_to(sq_part, (traits, LANES))
        x_copy = remote(x_send, x_recv, pair_send.at[1], pair_recv.at[1], mate)
        x_copy.start()
        if last:
            e_copy = remote(coef, e_recv, pair_send.at[2], pair_recv.at[2], mate)
            d_copy = remote(dir_low, ed_recv, pair_send.at[3], pair_recv.at[3], mate)
            e_copy.start()
            d_copy.start()
        x_copy.wait()
        image = mask * (image_part + x_recv[:, :people])
        dir_sq = sq_part + x_recv[:, people : people + 1]
        image_low = image.astype(BF16)
        dot_row = to_row(jnp.sum(image_low.astype(F32) * image, axis=1, keepdims=True), 0)
        if not last:
            send_pd(dot_row)
            copies = reduce_scatter(image_low, rs_send, rs_recv, False)

            @pl.when(owner)
            def _():
                pd = to_col(owner_pd(), 0)
                step = norm / (pd / noise_var + ridge * dir_sq)
                applied = owner_sum(rs_send, rs_recv, False) / noise_var + ridge * dir_low[:, pl.ds(own_col, chunk)].astype(F32)
                fresh = search[...] - step * applied
                search[...] = fresh
                owner_gather(to_row(jnp.sum(fresh * fresh, axis=1, keepdims=True), 0) + to_row(step, 1))

            totals, head = wait_gather()
            norm_next = to_col(totals, 0)
            step = to_col(head, 1)
            ratio = norm_next / norm
            norm = norm_next
            coef[...] += step * wide
            residual = residual - step * image
            for o in range(owners):
                cols = slice(o * chunk, (o + 1) * chunk)
                fresh = ag_recv[o].astype(F32) + ratio * dir_full[:, cols]
                dir_full[:, cols] = fresh
                dir_low[:, cols] = fresh.astype(BF16)
            finish(copies, pd_copy)

    row = (
        dot_row
        + to_row(jnp.sum(residual * image, axis=1, keepdims=True), 1)
        + to_row(jnp.sum(residual * residual, axis=1, keepdims=True), 2)
        + to_row(jnp.sum(image * image, axis=1, keepdims=True), 3)
    )
    pd_send[0:1, :] = row

    def f_copy(slot, k):
        return remote(
            pd_send.at[pl.ds(0, 1), :], f_recv.at[slot, pl.ds(0, 1), :], f_ssem.at[k], f_rsem.at[slot], 2 * k + core
        )

    for k in range(chips):

        @pl.when(chip != k)
        def _():
            f_copy(chip, k).start()

    f_recv[chip, 0:1, :] = row
    e_copy.wait()
    d_copy.wait()
    for k in range(chips):

        @pl.when(chip != k)
        def _():
            f_copy(k, 0).wait_recv()

    total = f_recv[0, 0:1, :]
    for k in range(1, chips):
        total = total + f_recv[k, 0:1, :]
    step = norm / (to_col(total, 0) / noise_var + ridge * dir_sq)
    squares = to_col(total, 2) - 2.0 * step * to_col(total, 1) + step * step * to_col(total, 3)
    residual_new = residual - step * image
    res_out[...] = jnp.where(core == 0, residual_new[:, :rows], residual_new[:, rows:])
    present = counts_ref[0]
    for d in range(1, n):
        present = present + counts_ref[d]
    sigma = (squares + PRIOR_DOF * PRIOR_SCALE) / ((present.astype(F32) + PRIOR_DOF) * small(gamma_ref))
    sigma_out[...] = to_row(sigma, 0)[:, :traits]
    new_mine = coef[...] + step * wide
    new_theirs = e_recv[...] + step * ed_recv[...].astype(F32)
    for b in range(width // batch):
        for offset, value in ((mine, new_mine), (theirs, new_theirs)):
            cols = pl.ds(pl.multiple_of(offset + b * batch, LANES), half)
            coef_out[:, cols] = jnp.where(block_ref[0] == b, value, coef_v[:, cols])
    for k in range(chips):

        @pl.when(chip != k)
        def _():
            f_copy(chip, k).wait_send()


def per_device(
    n,
    genotypes,
    residual,
    noise_people,
    noise_coef,
    coef_all,
    block_index,
    prior_prec,
    sigma2_old,
    gamma_draw,
    valid_counts,
):
    rows, batch = genotypes.shape
    traits, width = coef_all.shape
    half = batch // 2
    people = 2 * rows
    chips = n // 2
    owners = max(1, min(chips, half // LANES))
    chunk = half // owners
    vmem = pl.BlockSpec(memory_space=pltpu.VMEM)
    hbm = pl.BlockSpec(memory_space=pltpu.HBM)
    dma = pltpu.SemaphoreType.DMA
    coef_new, residual_new, sigma = pl.pallas_call(
        functools.partial(kernel, n, owners),
        out_shape=(
            jax.ShapeDtypeStruct((traits, width), F32),
            jax.ShapeDtypeStruct((traits, rows), F32),
            jax.ShapeDtypeStruct((1, traits), F32),
        ),
        in_specs=[hbm] * 10,
        out_specs=(vmem, vmem, vmem),
        scratch_shapes=[
            pltpu.SMEM(block_index.shape, jnp.int32),
            pltpu.SMEM(valid_counts.shape, jnp.int32),
            pltpu.VMEM((1, traits), F32),
            pltpu.VMEM((1, traits), F32),
            pltpu.VMEM((1, traits), F32),
            pltpu.VMEM((traits, rows), F32),
            pltpu.VMEM((traits, rows), F32),
            pltpu.VMEM((people, half), BF16),
            pltpu.VMEM((rows, half), BF16),
            pltpu.VMEM((traits, width), F32),
            pltpu.VMEM((traits, chunk), F32),
            pltpu.VMEM((traits, half), BF16),
            pltpu.VMEM((traits, half), F32),
            pltpu.VMEM((traits, half), F32),
            pltpu.VMEM((traits, chunk), F32),
            pltpu.VMEM((traits, rows), BF16),
            pltpu.VMEM((traits, rows), BF16),
            pltpu.VMEM((traits, rows), F32),
            pltpu.VMEM((traits, rows), F32),
            pltpu.VMEM((traits, people + LANES), F32),
            pltpu.VMEM((traits, people + LANES), F32),
            pltpu.VMEM((owners, traits, chunk), BF16),
            pltpu.VMEM((chips, traits, chunk), BF16),
            pltpu.VMEM((owners, traits, chunk), jnp.int16),
            pltpu.VMEM((chips, traits, chunk), jnp.int16),
            pltpu.VMEM((owners, 8, LANES), F32),
            pltpu.VMEM((8, LANES), F32),
            pltpu.VMEM((chips, 8, LANES), F32),
            pltpu.VMEM((traits, chunk), BF16),
            pltpu.VMEM((owners, traits, chunk), BF16),
            pltpu.VMEM((8, LANES), F32),
            pltpu.VMEM((2 * owners, 8, LANES), F32),
            pltpu.VMEM((chips, 8, LANES), F32),
            pltpu.VMEM((traits, half), F32),
            pltpu.VMEM((traits, half), BF16),
            dma((11,)),
            dma((4,)),
            dma((4,)),
            dma((owners,)),
            dma((chips,)),
            dma((owners,)),
            dma((chips,)),
            dma((chips,)),
            dma((owners,)),
            dma((n,)),
            dma((2 * owners,)),
            dma((chips,)),
            dma((chips,)),
        ],
        compiler_params=pltpu.CompilerParams(
            collective_id=0, has_side_effects=True, vmem_limit_bytes=60 * 1024 * 1024
        ),
    )(
        block_index,
        valid_counts,
        prior_prec[None, :],
        sigma2_old[None, :],
        gamma_draw[None, :],
        residual,
        noise_people,
        noise_coef,
        coef_all,
        genotypes,
    )
    return (coef_new, residual_new, sigma.reshape(traits))


def solution(mesh):
    return jax.shard_map(
        functools.partial(per_device, mesh.shape["ppl"]),
        mesh=mesh,
        in_specs=(
            P(("trait", "ppl"), None),
            P("trait", "ppl"),
            P("trait", "ppl"),
            P("trait", None),
            P("trait", None),
            P("trait"),
            P("trait"),
            P("trait"),
            P("trait"),
            P("trait"),
        ),
        out_specs=(P("trait", None), P("trait", "ppl"), P("trait")),
        check_vma=False,
    )
```
